8 devices in a mesh: dp: 1 (over z), tp: 8 (over x, y, core).
Axes of the slice: x: 2, y: 2, z: 1, core: 2. Of those that a mesh axis runs over, the one named last changes fastest.
Arguments:
- x: bfloat16 [4, 512, 5120], P('dp')
- gain_a: bfloat16 [5120], replicated
- wq: bfloat16 [5120, 8192], P(None, 'tp')
- wk: bfloat16 [5120, 1024], P(None, 'tp')
- wv: bfloat16 [5120, 1024], P(None, 'tp')
- wo: bfloat16 [8192, 5120], P('tp')
- gain_m: bfloat16 [5120], replicated
- w_gate: bfloat16 [5120, 25600], P(None, 'tp')
- w_up: bfloat16 [5120, 25600], P(None, 'tp')
- w_down: bfloat16 [25600, 5120], P('tp')
Outputs:
- output: bfloat16 [4, 512, 5120], P('dp')
All inputs are finite; a program needn't handle non-finite values.
Results may differ from the reference program's by a relative error of at most 0.017.
Values are sent between devices in bfloat16 or wider.
A program may use at most 2 GiB of HBM per device.

```python
import jax
import jax.numpy as jnp
from jax import lax

SEQUENCES = 4
TOKENS = 512
D = 5120
HEADS = 64
KV_HEADS = 8
HEAD = 128
FF = 25600
THETA = 10000


def setup_inputs(seed: int = 0, part: int = 0) -> dict:
    kx, ka, km, kq, kk, kv, ko, kg, ku, kd = jax.random.split(jax.random.key(seed), 10)

    def weights(key, rows, columns):
        return jax.random.normal(key, (rows, columns), jnp.float32) * rows**-0.5

    drawn = {
        "x": jax.random.normal(jax.random.fold_in(kx, part), (SEQUENCES, TOKENS, D), jnp.float32),
        "gain_a": 1 + 0.1 * jax.random.normal(ka, (D,), jnp.float32),
        "wq": 2 * weights(kq, D, HEADS * HEAD),
        "wk": 2 * weights(kk, D, KV_HEADS * HEAD),
        "wv": 4 * weights(kv, D, KV_HEADS * HEAD),
        "wo": weights(ko, HEADS * HEAD, D),
        "gain_m": 1 + 0.1 * jax.random.normal(km, (D,), jnp.float32),
        "w_gate": weights(kg, D, FF),
        "w_up": weights(ku, D, FF),
        "w_down": 3 * weights(kd, FF, D),
    }
    return {k: v.astype(jnp.bfloat16) for k, v in drawn.items()}


def normed(x, gain):
    wide = x.astype(jnp.float32)
    scale = lax.rsqrt(jnp.mean(wide * wide, -1, keepdims=True) + 1e-6)
    return (wide * scale * gain.astype(jnp.float32)).astype(jnp.bfloat16)


def turned(t, place, theta):
    half = t.shape[-1] // 2
    angle = place.astype(jnp.float32)[:, None] * theta ** (-jnp.arange(half, dtype=jnp.float32) / half)
    cos, sin = jnp.cos(angle)[:, None], jnp.sin(angle)[:, None]
    a, b = t[..., :half].astype(jnp.float32), t[..., half:].astype(jnp.float32)
    return jnp.concatenate([a * cos - b * sin, b * cos + a * sin], -1).astype(jnp.bfloat16)


def matmul(a, w):
    return jnp.dot(a, w, preferred_element_type=jnp.float32).astype(jnp.bfloat16)


def einsum(form, a, b):
    return jnp.einsum(form, a.astype(jnp.float32), b.astype(jnp.float32))


def attention(q, k, v):
    scores = einsum("tgsd,ugd->gstu", q, k) * q.shape[-1] ** -0.5
    token = jnp.arange(q.shape[0])
    scores = jnp.where(token[:, None] >= token, scores, -jnp.inf)
    weights = jax.nn.softmax(scores, -1).astype(jnp.bfloat16)
    return einsum("gstu,ugd->tgsd", weights, v).astype(jnp.bfloat16)


def one(x, gain_a, wq, wk, wv, wo, gain_m, w_gate, w_up, w_down):
    rows = x.shape[0]
    a, place = normed(x, gain_a), jnp.arange(rows)
    k = turned(matmul(a, wk).reshape(rows, -1, HEAD), place, THETA)
    q = turned(matmul(a, wq).reshape(rows, -1, HEAD), place, THETA).reshape(rows, k.shape[1], -1, HEAD)
    v = matmul(a, wv).reshape(rows, -1, HEAD)
    seen = attention(q, k, v).reshape(rows, -1)
    h = (x.astype(jnp.float32) + jnp.dot(seen, wo, preferred_element_type=jnp.float32)).astype(jnp.bfloat16)
    b = normed(h, gain_m)
    gate = jnp.dot(b, w_gate, preferred_element_type=jnp.float32)
    up = jnp.dot(b, w_up, preferred_element_type=jnp.float32)
    hidden = (jax.nn.silu(gate) * up).astype(jnp.bfloat16)
    return (h.astype(jnp.float32) + jnp.dot(hidden, w_down, preferred_element_type=jnp.float32)).astype(jnp.bfloat16)


def reference(x, gain_a, wq, wk, wv, wo, gain_m, w_gate, w_up, w_down):
    return lax.map(lambda sequence: one(sequence, gain_a, wq, wk, wv, wo, gain_m, w_gate, w_up, w_down), x)
```

```python
import functools

import jax
import jax.numpy as jnp
from jax import lax
from jax.experimental import pallas as pl
from jax.experimental.pallas import tpu as pltpu
from jax.sharding import PartitionSpec as P

BF, F32 = jnp.bfloat16, jnp.float32
HEAD = 128
THETA = 10000
LOG2E = 1.4426950408889634
HIDDEN = -2e30
MESH = pl.DeviceIdType.MESH
VMEM = 67043328 - 2**19

NS = 3
T, D, FF = 512, 5120, 3200
HEADS = 8
QKV = 5
GU = FF // 128
DN = 10
B = 4
FIRST = (4, 2)
SECOND = (2, 4)


def _rows(i, n):
    return pl.ds(pl.multiple_of(i, n), n)


def _kernel(events, x, gain_a, wq, wk, wv, wo, gain_m, wg, wu, wd, cos, sin, z, a, hid, vt, gu, dn, own, s0, r0, pk, sb1, r1, sb2, r2, ob, hp,
            xp, xs, gu_sem, dn_sem, s0_send, s0_recv, s1_send, s1_recv, s2_send, s2_recv, ag_send, ag_recv, x_sem, xp_sem, ld_sem):
    me = lax.axis_index("tp")
    core, yb, xb = lax.rem(me, 2), lax.rem(lax.div(me, 2), 2), lax.div(me, 4)
    bits = ((xb, yb), (yb, xb))

    def row(k, cc, part, b1, b2):
        return k * T + cc * 256 + part * 128 + b1 * 64 + b2 * 32

    def remote(src, dst, send, recv, mask):
        return pltpu.make_async_remote_copy(src_ref=src, dst_ref=dst, send_sem=send, recv_sem=recv, device_id={"tp": jnp.bitwise_xor(me, mask)},
                                            device_id_type=MESH)


    def gu_copies(src, col0, src1, col1, slot):
        return (pltpu.make_async_copy(src.at[:, pl.ds(pl.multiple_of(col0, 128), 128)], gu.at[slot, :, pl.ds(0, 128)], gu_sem.at[slot, 0]),
                pltpu.make_async_copy(src1.at[:, pl.ds(pl.multiple_of(col1, 128), 128)], gu.at[slot, :, pl.ds(128, 128)], gu_sem.at[slot, 1]))

    def gu_start(g):
        slot = lax.rem(g, NS)

        @pl.when(g < B * QKV)
        def _():
            t = lax.rem(g, QKV)

            @pl.when(t < QKV - 1)
            def _():
                for c in gu_copies(wq, t * 256, wq, t * 256 + 128, slot):
                    c.start()

            @pl.when(t == QKV - 1)
            def _():
                for c in gu_copies(wk, 0, wv, 0, slot):
                    c.start()

        @pl.when((g >= B * QKV) & (g < B * (QKV + GU)))
        def _():
            t = lax.rem(g - B * QKV, GU)
            for c in gu_copies(wg, t * 128, wu, t * 128, slot):
                c.start()

    def gu_wait(g):
        slot = lax.rem(g, NS)
        for c in gu_copies(wg, 0, wu, 0, slot):
            c.wait()
        return slot

    def dn_copy(w, depth, t, slot):
        return pltpu.make_async_copy(w.at[:, pl.ds(pl.multiple_of(t * 512, 512), 512)], dn.at[slot, pl.ds(0, depth), :], dn_sem.at[slot])

    def dn_start(g):
        slot, t = lax.rem(g, NS), lax.rem(g, DN)

        @pl.when(g < B * DN)
        def _():
            dn_copy(wo, HEADS * HEAD, t, slot).start()

        @pl.when((g >= B * DN) & (g < 2 * B * DN))
        def _():
            dn_copy(wd, FF, t, slot).start()


    def s0_copy(slot, t):
        cols = pl.ds(pl.multiple_of(t * 512, 512), 512)
        return remote(s0.at[:, cols], r0.at[slot, :, cols], s0_send.at[t], s0_recv.at[slot, t], 1)

    def s1_copy(slot, p):
        return remote(sb1.at[pl.ds(64 * p, 64)], r1.at[slot, pl.ds(64 * p, 64)], s1_send.at[p], s1_recv.at[slot, p], FIRST[p])

    def s2_copy(slot, p):
        return remote(sb2.at[pl.ds(32 * p, 32)], r2.at[slot, pl.ds(32 * p, 32)], s2_send.at[p], s2_recv.at[slot, p], SECOND[p])

    def xp_copy(k, p):
        return pltpu.make_async_copy(x.at[_rows(row(k, core, p, *bits[p]), 32)], xp.at[pl.ds(32 * p, 32)], xp_sem.at[p])

    def piece(k, p, kind):
        m1, m2 = bits[p]
        at = _rows(row(k, core, p, m1, m2), 32)
        src = ob.at[lax.rem(k, 2), pl.ds(32 * p, 32)]
        if kind in (2, 4):
            at = _rows(row(k, core, p, m1, 1 - m2), 32)
            src = z.at[at]
        if kind == 5:
            at = _rows(row(k, core, p, 1 - m1, 0), 64)
            src = z.at[at]
        return remote(src, z.at[at], ag_send.at[k, p, kind], ag_recv.at[k, p, kind], (SECOND[p], FIRST[p], FIRST[p], 1, 1, 1)[kind])

    def kept(k, p):
        return pltpu.make_async_copy(ob.at[lax.rem(k, 2), pl.ds(32 * p, 32)], z.at[_rows(row(k, core, p, *bits[p]), 32)], ag_send.at[k, p, 6])

    def e1(k):
        slot = lax.rem(k, 2)
        lax.fori_loop(0, DN, lambda t, _: s0_copy(slot, t).wait_recv(), None)

        @pl.when(k > 0)
        def _():
            for p in (0, 1):
                s1_copy(slot, p).wait_send()

        def send(n, _):
            here = _rows(128 + 16 * n, 16)
            sb1[_rows(16 * n, 16), :] = (own[here, :] + r0[slot, here, :].astype(F32)).astype(BF)

        lax.fori_loop(0, 8, send, None)
        for p in (0, 1):
            s1_copy(slot, p).start()

        def keep(n, _):
            here = _rows(16 * n, 16)
            pk[here, :] = own[here, :] + r0[slot, here, :].astype(F32)

        lax.fori_loop(0, 8, keep, None)

    def e2(k):
        slot = lax.rem(k, 2)
        for p in (0, 1):
            s1_copy(slot, p).wait_recv()

        @pl.when(k > 0)
        def _():
            for p in (0, 1):
                s2_copy(slot, p).wait_send()

        def some(n, _):
            p, m = lax.div(n, 2), lax.rem(n, 2)
            here, there = _rows(p * 64 + m * 16, 16), _rows(p * 64 + 32 + m * 16, 16)
            sb2[_rows(p * 32 + m * 16, 16), :] = (pk[there, :] + r1[slot, there, :].astype(F32)).astype(BF)
            pk[here, :] = pk[here, :] + r1[slot, here, :].astype(F32)

        lax.fori_loop(0, 4, some, None)
        for p in (0, 1):
            s2_copy(slot, p).start()

        @pl.when(k < B)
        def _():
            for p in (0, 1):
                xp_copy(k, p).start()

    def e3(k):
        slot = lax.rem(k, 2)
        for p in (0, 1):
            s2_copy(slot, p).wait_recv()

        @pl.when(k >= 2)
        def _():
            for p in (0, 1):
                for kind in (0, 1, 3):
                    piece(k - 2, p, kind).wait_send()

        def total(n):
            p, m = lax.div(n, 2), lax.rem(n, 2)
            return pk[_rows(p * 64 + m * 16, 16), :] + r2[slot, _rows(n * 16, 16), :].astype(F32)

        @pl.when(k < B)
        def _():
            for p in (0, 1):
                xp_copy(k, p).wait()

            def some(n, _):
                here = _rows(n * 16, 16)
                h = (xp[here, :].astype(F32) + total(n)).astype(BF)
                hp[k, here, :] = h
                wide = h.astype(F32)
                scale = lax.rsqrt(jnp.mean(wide * wide, -1, keepdims=True) + 1e-6)
                ob[slot, here, :] = (wide * scale * gain_m[...].astype(F32)).astype(BF)

            lax.fori_loop(0, 4, some, None)

        @pl.when(k >= B)
        def _():
            def some(n, _):
                here = _rows(n * 16, 16)
                ob[slot, here, :] = (hp[k - B, here, :].astype(F32) + total(n)).astype(BF)

            lax.fori_loop(0, 4, some, None)

        for kind in (0, 1, 3):
            for p in (0, 1):
                piece(k, p, kind).start()
        for p in (0, 1):
            kept(k, p).start()

    def e4(k):
        for p in (0, 1):
            piece(k, p, 0).wait_recv()
            piece(k, p, 2).start()
        for p in (0, 1):
            piece(k, p, 4).start()
            kept(k, p).wait()

    def e5(k):
        for p in (0, 1):
            piece(k, p, 1).wait_recv()
            piece(k, p, 2).wait_recv()
            piece(k, p, 5).start()

    def e6(k):
        for p in (0, 1):
            for kind in (3, 4, 5):
                piece(k, p, kind).wait_recv()
            for kind in (2, 4, 5):
                piece(k, p, kind).wait_send()

    def load(k):
        e6(k)

        def some(n, _):
            sc, s1, p, s2 = lax.div(n, 8), lax.rem(lax.div(n, 4), 2), lax.rem(lax.div(n, 2), 2), lax.rem(n, 2)
            m1, m2 = jnp.where(p == 0, xb, yb), jnp.where(p == 0, yb, xb)
            flip = lambda b, s: b + s - 2 * b * s
            at = row(k, flip(core, sc), p, flip(m1, s1), flip(m2, s2))
            pltpu.make_async_copy(z.at[_rows(at, 32)], a.at[_rows(n * 32, 32)], ld_sem).start()

        lax.fori_loop(0, 16, some, None)

    steps = {"e5": e5, "e4": e4, "e3": e3, "e2": e2, "e1": e1, "ld": load}

    def hook(loop, g):
        for kind in events["order"]:
            step = steps[kind]
            at = [(w, k) for w, e, k in events.get(loop, ()) if e == kind]
            if at:
                hit, k = g == at[0][0], jnp.where(g == at[0][0], at[0][1], 0)
                for w, n in at[1:]:
                    hit, k = hit | (g == w), jnp.where(g == w, n, k)
                pl.when(hit)(functools.partial(step, k))


    def x_copy(i, n):
        return pltpu.make_async_copy(x.at[_rows(i * T + n * 64, 64)], xs.at[lax.rem(n, 2)], x_sem.at[lax.rem(n, 2)])

    def norm(i):
        def some(n, _):
            x_copy(i, n).wait()
            for m in range(4):
                wide = xs[lax.rem(n, 2), 16 * m : 16 * m + 16, :].astype(F32)
                scale = lax.rsqrt(jnp.mean(wide * wide, -1, keepdims=True) + 1e-6)
                a[_rows(n * 64 + 16 * m, 16), :] = (wide * scale * gain_a[...].astype(F32)).astype(BF)

            @pl.when(n < 6)
            def _():
                x_copy(i, n + 2).start()

        lax.fori_loop(0, 8, some, None)

    def project(i):
        def tile(t, _):
            g = i * QKV + t
            gu_start(g + NS - 1)
            slot = gu_wait(g)
            y = jnp.dot(a[...], gu[slot], preferred_element_type=F32).astype(BF)

            def turned(v):
                w = v.astype(F32)
                return (w * cos[...] + pltpu.roll(w, 64, 1) * sin[...]).astype(BF)

            left, right = y[:, :128], y[:, 128:]
            hid[:, pl.ds(pl.multiple_of(t * 256, 256), 128)] = turned(left)
            hid[:, pl.ds(pl.multiple_of(t * 256 + 128, 128), 128)] = jnp.where(t == QKV - 1, right, turned(right))
            hook("qkv", g)

        lax.fori_loop(0, QKV, tile, None)
        vt[...] = hid[:, HEADS * HEAD + HEAD : HEADS * HEAD + 2 * HEAD].T

    def attention(i):
        e = HEAD**-0.5 * LOG2E
        visible = lax.rem(lax.broadcasted_iota(jnp.int32, (128, 256), 1), 128) >= lax.broadcasted_iota(jnp.int32, (128, 256), 0)

        def pair(n, _):
            here = pl.ds(pl.multiple_of(n * 256, 256), 256)
            for j in range(4):
                keys = 128 * (j + 1)
                q = hid[128 * j : 128 * j + 128, here]
                q = jnp.concatenate([q[:, :128], q[:, 128:]], axis=0)
                k = hid[:keys, HEADS * HEAD : HEADS * HEAD + HEAD]
                s = lax.dot_general(k, q, (((1,), (1,)), ((), ())), preferred_element_type=F32)
                last = jnp.where(visible, s[keys - 128 :], HIDDEN)
                s = last if j == 0 else jnp.concatenate([s[: keys - 128], last], axis=0)
                p = jnp.exp2((s - s.max(axis=0, keepdims=True)) * e)
                out = jnp.dot(vt[:, :keys], p.astype(BF), preferred_element_type=F32) * (1 / p.sum(axis=0, keepdims=True))
                out = out.T.astype(BF)
                out = jnp.concatenate([out[:128], out[128:]], axis=1)
                cb, part = j // 2, j % 2
                flip = lambda b, s: (1 - s) if b else s
                for b1 in (0, 1):
                    for b2 in (0, 1):
                        m1, m2 = bits[part]
                        at = flip(cb, core) * 256 + flip(b1, m1) * 128 + part * 64 + flip(b2, m2) * 32
                        hid[_rows(at, 32), pl.ds(pl.multiple_of(2048 + n * 256, 256), 256)] = out[b1 * 64 + b2 * 32 : b1 * 64 + b2 * 32 + 32, :]

        lax.fori_loop(0, HEADS // 2, pair, None)

    def terms(i, k, lhs, depth, loop):
        slot = lax.rem(k, 2)

        def tile(t, _):
            g = k * DN + t
            dn_start(g + NS - 1)
            dn_copy(wo if depth == HEADS * HEAD else wd, depth, t, lax.rem(g, NS)).wait()
            y = jnp.dot(lhs[...], dn[lax.rem(g, NS), :depth, :], preferred_element_type=F32)
            cols = pl.ds(pl.multiple_of(t * 512, 512), 512)

            @pl.when(k > 0)
            def _():
                s0_copy(slot, t).wait_send()

            own[:, cols] = y[:256]
            s0[:, cols] = y[256:].astype(BF)
            s0_copy(slot, t).start()
            hook(loop, i * DN + t)

        lax.fori_loop(0, DN, tile, None)

    def first_half(i, _):
        norm(i)
        hook("norm", i)
        project(i)

        @pl.when(i < B - 1)
        def _():
            for n in (0, 1):
                x_copy(i + 1, n).start()

        attention(i)
        hook("attn", i)
        terms(i, i, hid.at[:, pl.ds(2048, HEADS * HEAD)], HEADS * HEAD, "wo")

    def second_half(i, _):
        hook("m", i)
        pltpu.make_async_copy(z.at[pl.ds(0, T)], a, ld_sem).wait()

        def tile(t, _):
            g = B * QKV + i * GU + t
            gu_start(g + NS - 1)
            slot = gu_wait(g)
            y = jnp.dot(a[...], gu[slot], preferred_element_type=F32)
            gate, up = y[:, :128], y[:, 128:]
            hid[:, pl.ds(pl.multiple_of(t * 128, 128), 128)] = (gate * jax.nn.sigmoid(gate) * up).astype(BF)
            hook("gu", i * GU + t)

        lax.fori_loop(0, GU, tile, None)
        terms(i, B + i, hid, FF, "down")


    for n in (0, 1):
        x_copy(0, n).start()
    for g in range(NS - 1):
        gu_start(jnp.int32(g))
        dn_start(jnp.int32(g))
    barrier = pltpu.get_barrier_semaphore()
    for mask in (1, 2, 4):
        pl.semaphore_signal(barrier, inc=1, device_id={"tp": jnp.bitwise_xor(me, mask)}, device_id_type=MESH)
    pl.semaphore_wait(barrier, 3)

    lax.fori_loop(0, B, first_half, None)
    lax.fori_loop(0, B, second_half, None)
    for kind, k in events["end"]:
        steps[kind](jnp.int32(k))
    lax.fori_loop(B, 2 * B, lambda k, _: e6(k), None)
    lax.fori_loop(0, DN, lambda t, _: s0_copy(0, t).wait_send(), None)
    for p in (0, 1):
        s1_copy(0, p).wait_send()
        s2_copy(0, p).wait_send()
        for k in (2 * B - 2, 2 * B - 1):
            for kind in (0, 1, 3):
                piece(k, p, kind).wait_send()


def _table():
    ev = {"norm": [], "attn": [], "wo": [], "qkv": [], "gu": [], "down": [], "m": [], "end": []}
    for i in range(4):
        for e in ("e1", "e2", "e3", "e4", "e5"):
            if i < 3:
                ev["norm"].append((i + 1, e, i))
            else:
                ev["m"].append((0, e, i))
    ev["m"].append((0, "ld", 0))
    for i in range(1, 4):
        ev["down"].append((i * DN - 1, "ld", i))
    for i in range(3):
        for e in ("e1", "e2", "e3", "e4", "e5"):
            ev["m"].append((i + 1, e, 4 + i))
    ev["end"] = [(e, 7) for e in ("e1", "e2", "e3", "e4", "e5")]
    ev["order"] = ("e1", "e2", "e3", "e4", "e5", "ld")
    return ev


def solution(mesh):
    def step(x, gain_a, wq, wk, wv, wo, gain_m, w_gate, w_up, w_down):
        half = HEAD // 2
        angle = jnp.arange(T, dtype=F32)[:, None] * THETA ** (-jnp.arange(half, dtype=F32) / half)
        cos, sin = jnp.cos(angle), jnp.sin(angle)
        anywhere, vmem = pl.BlockSpec(memory_space=pl.ANY), pl.BlockSpec(memory_space=pltpu.VMEM)
        dma = pltpu.SemaphoreType.DMA
        z = pl.pallas_call(
            functools.partial(_kernel, _table()),
            out_shape=jax.ShapeDtypeStruct((2 * B * T, D), BF),
            in_specs=[anywhere, vmem, anywhere, anywhere, anywhere, anywhere, vmem, anywhere, anywhere, anywhere, vmem, vmem],
            out_specs=pl.BlockSpec(memory_space=pltpu.HBM),
            scratch_shapes=[
                pltpu.VMEM((T, D), BF), pltpu.VMEM((T, FF), BF), pltpu.VMEM((HEAD, T), BF),
                pltpu.VMEM((NS, D, 256), BF), pltpu.VMEM((NS, FF, 512), BF),
                pltpu.VMEM((256, D), F32), pltpu.VMEM((256, D), BF), pltpu.VMEM((2, 256, D), BF),
                pltpu.VMEM((128, D), F32), pltpu.VMEM((128, D), BF), pltpu.VMEM((2, 128, D), BF),
                pltpu.VMEM((64, D), BF), pltpu.VMEM((2, 64, D), BF),
                pltpu.VMEM((2, 64, D), BF), pltpu.VMEM((B, 64, D), BF), pltpu.VMEM((64, D), BF), pltpu.VMEM((2, 64, D), BF),
                dma((NS, 2)), dma((NS,)), dma((DN,)), dma((2, DN)), dma((2,)), dma((2, 2)), dma((2,)), dma((2, 2)),
                dma((2 * B, 2, 7)), dma((2 * B, 2, 6)), dma((2,)), dma((2,)), dma(()),
            ],
            compiler_params=pltpu.CompilerParams(collective_id=0, has_side_effects=True, vmem_limit_bytes=VMEM),
            name="layer",
        )(x.reshape(B * T, D), gain_a.reshape(1, D), wq, wk, wv, wo, gain_m.reshape(1, D), w_gate, w_up, w_down,
          jnp.concatenate([cos, cos], -1), jnp.concatenate([-sin, sin], -1))
        return z[B * T :].reshape(x.shape)

    tokens, whole, columns, rows_of = P("dp", None, None), P(None), P(None, "tp"), P("tp", None)
    return jax.shard_map(
        step,
        mesh=mesh,
        in_specs=(tokens, whole, columns, columns, columns, rows_of, whole, columns, columns, rows_of),
        out_specs=tokens,
        check_vma=False,
    )
```

```python
import functools

import jax
import jax.numpy as jnp
from jax import lax
from jax.experimental import pallas as pl
from jax.experimental.pallas import tpu as pltpu
from jax.sharding import PartitionSpec as P

BF, F32 = jnp.bfloat16, jnp.float32
HEAD = 128
THETA = 10000
LOG2E = 1.4426950408889634
HIDDEN = -2e30
MESH = pl.DeviceIdType.MESH
VMEM = 67043328 - 2**19

NS = 3
T, D, FF = 512, 5120, 3200
HEADS = 8
QKV = 3
GU = 13
DN = 10
B = 4
FIRST = (4, 2)
SECOND = (2, 4)
KEYS = slice(HEADS * HEAD, HEADS * HEAD + HEAD)
SEEN = 2048


def _rows(i, n):
    return pl.ds(pl.multiple_of(i, n), n)


def _kernel(events, x, gain_a, wq, wk, wv, wo, gain_m, wg, wu, wd, cos, sin, z, a, hid, vt, gu, dn, own, s0, r0, pk, sb1, r1, sb2, r2, ob, hp,
            xp, xs, gu_sem, dn_sem, s0_send, s0_recv, s1_send, s1_recv, s2_send, s2_recv, ag_send, ag_recv, x_sem, xp_sem, ld_sem):
    me = lax.axis_index("tp")
    core, yb, xb = lax.rem(me, 2), lax.rem(lax.div(me, 2), 2), lax.div(me, 4)
    bits = ((xb, yb), (yb, xb))

    def row(k, cc, part, b1, b2):
        return k * T + cc * 256 + part * 128 + b1 * 64 + b2 * 32

    def remote(src, dst, send, recv, mask):
        return pltpu.make_async_remote_copy(src_ref=src, dst_ref=dst, send_sem=send, recv_sem=recv, device_id={"tp": jnp.bitwise_xor(me, mask)},
                                            device_id_type=MESH)


    def gu_copies(slot, n, one, at, other, there):
        return (pltpu.make_async_copy(one.at[:, pl.ds(pl.multiple_of(at, 128), n)], gu.at[slot, :, pl.ds(0, n)], gu_sem.at[slot, 0]),
                pltpu.make_async_copy(other.at[:, pl.ds(pl.multiple_of(there, 128), n)], gu.at[slot, :, pl.ds(n, n)], gu_sem.at[slot, 1]))

    def gu_start(g):
        slot = lax.rem(g, 2)
        attn = g < B * QKV
        t = jnp.where(attn, lax.rem(g, QKV), lax.rem(g - B * QKV, GU))
        for hit, n, one, at, other, there in (
            (attn & (t < QKV - 1), 256, wq, t * 512, wq, t * 512 + 256),
            (attn & (t == QKV - 1), 128, wk, 0, wv, 0),
            (~attn & (t < GU - 1) & (g < B * (QKV + GU)), 256, wg, t * 256, wu, t * 256),
            (~attn & (t == GU - 1), 128, wg, t * 256, wu, t * 256),
        ):

            @pl.when(hit)
            def _():
                for c in gu_copies(slot, n, one, at, other, there):
                    c.start()

    def gu_step(g, lhs, n):
        gu_start(g + 1)
        slot = lax.rem(g, 2)
        for c in gu_copies(slot, n, wg, 0, wu, 0):
            c.wait()
        return jnp.dot(lhs[...], gu[slot, :, : 2 * n], preferred_element_type=F32)

    def dn_copies(g, attn):
        slot = lax.rem(g, NS)

        def one(w, t, depth, at, n):
            return pltpu.make_async_copy(w.at[:, pl.ds(pl.multiple_of(t * 512, 512), 512)], dn.at[slot, pl.ds(at, depth), :], dn_sem.at[slot, n])

        if attn:
            t = lax.rem(g, DN // 2)
            return one(wo, 2 * t, HEADS * HEAD, 0, 0), one(wo, 2 * t + 1, HEADS * HEAD, HEADS * HEAD, 1)
        return (one(wd, lax.rem(g - B * DN // 2, DN), FF, 0, 0),)

    def dn_start(g):
        for attn, hit in ((True, g < B * DN // 2), (False, (g >= B * DN // 2) & (g < B * DN // 2 + B * DN))):

            @pl.when(hit)
            def _():
                for c in dn_copies(g, attn):
                    c.start()


    def s0_copy(slot, t):
        cols = pl.ds(pl.multiple_of(t * 512, 512), 512)
        return remote(s0.at[:, cols], r0.at[slot, :, cols], s0_send.at[t], s0_recv.at[slot, t], 1)

    def s1_copy(slot, p):
        return remote(sb1.at[pl.ds(64 * p, 64)], r1.at[slot, pl.ds(64 * p, 64)], s1_send.at[p], s1_recv.at[slot, p], FIRST[p])

    def s2_copy(slot, p):
        return remote(sb2.at[pl.ds(32 * p, 32)], r2.at[slot, pl.ds(32 * p, 32)], s2_send.at[p], s2_recv.at[slot, p], SECOND[p])

    def xp_copy(k, p):
        return pltpu.make_async_copy(x.at[_rows(row(k, core, p, *bits[p]), 32)], xp.at[lax.rem(k, 2), pl.ds(32 * p, 32)], xp_sem.at[lax.rem(k, 2), p])

    def piece(k, p, kind):
        m1, m2 = bits[p]
        at = _rows(row(k, core, p, m1, m2), 32)
        src = ob.at[lax.rem(k, 2), pl.ds(32 * p, 32)]
        if kind in (2, 4):
            at = _rows(row(k, core, p, m1, 1 - m2), 32)
            src = z.at[at]
        if kind == 5:
            at = _rows(row(k, core, p, 1 - m1, 0), 64)
            src = z.at[at]
        return remote(src, z.at[at], ag_send.at[k, p, kind], ag_recv.at[k, p, kind], (SECOND[p], FIRST[p], FIRST[p], 1, 1, 1)[kind])

    def kept(k, p):
        return pltpu.make_async_copy(ob.at[lax.rem(k, 2), pl.ds(32 * p, 32)], z.at[_rows(row(k, core, p, *bits[p]), 32)], ag_send.at[k, p, 6])

    def e1(k):
        slot = lax.rem(k, 2)
        lax.fori_loop(0, DN, lambda t, _: s0_copy(slot, t).wait_recv(), None)

        @pl.when(k > 0)
        def _():
            for p in (0, 1):
                s1_copy(slot, p).wait_send()

        def send(n, _):
            here = _rows(128 + 16 * n, 16)
            sb1[_rows(16 * n, 16), :] = (own[here, :] + r0[slot, here, :].astype(F32)).astype(BF)

        lax.fori_loop(0, 8, send, None)
        for p in (0, 1):
            s1_copy(slot, p).start()

        def keep(n, _):
            here = _rows(16 * n, 16)
            pk[slot, here, :] = own[here, :] + r0[slot, here, :].astype(F32)

        lax.fori_loop(0, 8, keep, None)

    def e2(k):
        slot = lax.rem(k, 2)
        for p in (0, 1):
            s1_copy(slot, p).wait_recv()

        @pl.when(k > 0)
        def _():
            for p in (0, 1):
                s2_copy(slot, p).wait_send()

        def some(n, _):
            p, m = lax.div(n, 2), lax.rem(n, 2)
            here, there = _rows(p * 64 + m * 16, 16), _rows(p * 64 + 32 + m * 16, 16)
            sb2[_rows(p * 32 + m * 16, 16), :] = (pk[slot, there, :] + r1[slot, there, :].astype(F32)).astype(BF)
            pk[slot, here, :] = pk[slot, here, :] + r1[slot, here, :].astype(F32)

        lax.fori_loop(0, 4, some, None)
        for p in (0, 1):
            s2_copy(slot, p).start()

        @pl.when(k < B)
        def _():
            for p in (0, 1):
                xp_copy(k, p).start()

    def e3(k):
        slot = lax.rem(k, 2)
        for p in (0, 1):
            s2_copy(slot, p).wait_recv()

        @pl.when(k >= 2)
        def _():
            for p in (0, 1):
                for kind in (0, 1, 3):
                    piece(k - 2, p, kind).wait_send()

        def total(n):
            p, m = lax.div(n, 2), lax.rem(n, 2)
            return pk[slot, _rows(p * 64 + m * 16, 16), :] + r2[slot, _rows(n * 16, 16), :].astype(F32)

        @pl.when(k < B)
        def _():
            for p in (0, 1):
                xp_copy(k, p).wait()

            def some(n, _):
                here = _rows(n * 16, 16)
                h = (xp[slot, here, :].astype(F32) + total(n)).astype(BF)
                hp[k, here, :] = h
                wide = h.astype(F32)
                scale = lax.rsqrt(jnp.mean(wide * wide, -1, keepdims=True) + 1e-6)
                ob[slot, here, :] = (wide * scale * gain_m[...].astype(F32)).astype(BF)

            lax.fori_loop(0, 4, some, None)

        @pl.when(k >= B)
        def _():
            def some(n, _):
                here = _rows(n * 16, 16)
                ob[slot, here, :] = (hp[k - B, here, :].astype(F32) + total(n)).astype(BF)

            lax.fori_loop(0, 4, some, None)

        for kind in (0, 1, 3):
            for p in (0, 1):
                piece(k, p, kind).start()
        for p in (0, 1):
            kept(k, p).start()

    def e4(k):
        for p in (0, 1):
            piece(k, p, 0).wait_recv()
            piece(k, p, 2).start()
        for p in (0, 1):
            piece(k, p, 4).start()
            kept(k, p).wait()

    def e5(k):
        for p in (0, 1):
            piece(k, p, 1).wait_recv()
            piece(k, p, 2).wait_recv()
            piece(k, p, 5).start()

    def e6(k):
        for p in (0, 1):
            for kind in (3, 4, 5):
                piece(k, p, kind).wait_recv()
            for kind in (2, 4, 5):
                piece(k, p, kind).wait_send()

    def load(k):
        e6(k)

        def some(n, _):
            sc, s1, p, s2 = lax.div(n, 8), lax.rem(lax.div(n, 4), 2), lax.rem(lax.div(n, 2), 2), lax.rem(n, 2)
            m1, m2 = jnp.where(p == 0, xb, yb), jnp.where(p == 0, yb, xb)
            flip = lambda b, s: b + s - 2 * b * s
            at = row(k, flip(core, sc), p, flip(m1, s1), flip(m2, s2))
            pltpu.make_async_copy(z.at[_rows(at, 32)], a.at[_rows(n * 32, 32)], ld_sem).start()

        lax.fori_loop(0, 16, some, None)

    steps = {"e5": e5, "e4": e4, "e3": e3, "e2": e2, "e1": e1, "ld": load}

    def hook(loop, g):
        for kind in events["order"]:
            step = steps[kind]
            at = [(w, k) for w, e, k in events.get(loop, ()) if e == kind]
            if at:
                hit, k = g == at[0][0], jnp.where(g == at[0][0], at[0][1], 0)
                for w, n in at[1:]:
                    hit, k = hit | (g == w), jnp.where(g == w, n, k)
                pl.when(hit)(functools.partial(step, k))


    def x_copy(i, n):
        return pltpu.make_async_copy(x.at[_rows(i * T + n * 64, 64)], xs.at[lax.rem(n, 4)], x_sem.at[lax.rem(n, 4)])

    def norm(i):
        def some(n, _):
            x_copy(i, n).wait()
            for m in range(4):
                wide = xs[lax.rem(n, 4), 16 * m : 16 * m + 16, :].astype(F32)
                scale = lax.rsqrt(jnp.mean(wide * wide, -1, keepdims=True) + 1e-6)
                a[_rows(n * 64 + 16 * m, 16), :] = (wide * scale * gain_a[...].astype(F32)).astype(BF)

            @pl.when(n < 4)
            def _():
                x_copy(i, n + 4).start()

        lax.fori_loop(0, 8, some, None)

    def project(i):
        def turned(v):
            w = v.astype(F32)
            return (w * cos[...] + pltpu.roll(w, 64, 1) * sin[...]).astype(BF)

        def queries(t, _):
            g = i * QKV + t
            y = gu_step(g, a, 256).astype(BF)
            for n in range(4):
                hid[:, pl.ds(pl.multiple_of(t * 512 + n * 128, 128), 128)] = turned(y[:, n * 128 : n * 128 + 128])
            hook("qkv", g)

        lax.fori_loop(0, QKV - 1, queries, None)
        y = gu_step(i * QKV + QKV - 1, a, 128).astype(BF)
        hid[:, KEYS] = turned(y[:, :128])
        vt[...] = y[:, 128:].T

    def attention(i):
        e = HEAD**-0.5 * LOG2E
        visible = lax.rem(lax.broadcasted_iota(jnp.int32, (128, 256), 1), 128) >= lax.broadcasted_iota(jnp.int32, (128, 256), 0)

        def pair(n, _):
            here = pl.ds(pl.multiple_of(n * 256, 256), 256)
            scores, weights, sums = [], [], []
            for j in range(4):
                keys = 128 * (j + 1)
                q = hid[128 * j : keys, here]
                q = jnp.concatenate([q[:, :128], q[:, 128:]], axis=0)
                scores.append(lax.dot_general(hid[:keys, KEYS], q, (((1,), (1,)), ((), ())), preferred_element_type=F32))
            for s in scores:
                before = s.shape[0] - 128
                last = jnp.where(visible, s[before:], HIDDEN)
                s = jnp.concatenate([s[:before], last], axis=0) if before else last
                p = jnp.exp2((s - s.max(axis=0, keepdims=True)) * e)
                sums.append(p.sum(axis=0, keepdims=True))
                weights.append(p.astype(BF))
            for j, (p, total) in enumerate(zip(weights, sums)):
                out = jnp.dot(vt[:, : 128 * (j + 1)], p, preferred_element_type=F32) * (1 / total)
                out = out.T.astype(BF)
                out = jnp.concatenate([out[:128], out[128:]], axis=1)
                cb, part = j // 2, j % 2
                flip = lambda b, s: (1 - s) if b else s
                for b1 in (0, 1):
                    for b2 in (0, 1):
                        m1, m2 = bits[part]
                        at = flip(cb, core) * 256 + flip(b1, m1) * 128 + part * 64 + flip(b2, m2) * 32
                        hid[_rows(at, 32), pl.ds(pl.multiple_of(SEEN + n * 256, 256), 256)] = out[b1 * 64 + b2 * 32 : b1 * 64 + b2 * 32 + 32, :]

        lax.fori_loop(0, HEADS // 2, pair, None)

    def terms(i, attn):
        k = i if attn else B + i
        steps = DN // 2 if attn else DN
        wide = DN // steps

        def step(t, _):
            g = i * steps + t + (0 if attn else B * DN // 2)
            slot = lax.rem(g, NS)
            dn_start(g + NS - 1)
            for c in dn_copies(g, attn):
                c.wait()
            if attn:
                ys = [jnp.dot(hid[:, SEEN : SEEN + HEADS * HEAD], dn[slot, n * HEADS * HEAD : (n + 1) * HEADS * HEAD, :], preferred_element_type=F32) for n in (0, 1)]
            else:
                ys = [jnp.dot(hid[...], dn[slot], preferred_element_type=F32)]
            for n, y in enumerate(ys):
                tile = t * wide + n
                cols = pl.ds(pl.multiple_of(tile * 512, 512), 512)

                @pl.when(k > 0)
                def _():
                    s0_copy(lax.rem(k, 2), tile).wait_send()

                own[:, cols] = y[:256]
                s0[:, cols] = y[256:].astype(BF)
                s0_copy(lax.rem(k, 2), tile).start()
            hook("wo" if attn else "down", i * steps + t)

        lax.fori_loop(0, steps, step, None)

    def first_half(i, _):
        norm(i)
        hook("norm", i)
        project(i)

        @pl.when(i < B - 1)
        def _():
            for n in range(4):
                x_copy(i + 1, n).start()

        attention(i)
        hook("attn", i)
        terms(i, True)

    def second_half(i, _):
        hook("m", i)
        pltpu.make_async_copy(z.at[pl.ds(0, T)], a, ld_sem).wait()

        def step(t, n):
            y = gu_step(B * QKV + i * GU + t, a, n)
            gate, up = y[:, :n], y[:, n:]
            hid[:, pl.ds(pl.multiple_of(t * 256, 256), n)] = (gate * jax.nn.sigmoid(gate) * up).astype(BF)
            hook("gu", i * GU + t)

        lax.fori_loop(0, GU - 1, lambda t, _: step(t, 256), None)
        step(jnp.int32(GU - 1), 128)
        terms(i, False)


    for n in range(4):
        x_copy(0, n).start()
    gu_start(jnp.int32(0))
    for g in range(NS - 1):
        dn_start(jnp.int32(g))
    barrier = pltpu.get_barrier_semaphore()
    for mask in (1, 2, 4):
        pl.semaphore_signal(barrier, inc=1, device_id={"tp": jnp.bitwise_xor(me, mask)}, device_id_type=MESH)
    pl.semaphore_wait(barrier, 3)

    lax.fori_loop(0, B, first_half, None)
    lax.fori_loop(0, B, second_half, None)
    for kind, k in events["end"]:
        steps[kind](jnp.int32(k))
    lax.fori_loop(B, 2 * B, lambda k, _: e6(k), None)
    lax.fori_loop(0, DN, lambda t, _: s0_copy(0, t).wait_send(), None)
    for p in (0, 1):
        s1_copy(0, p).wait_send()
        s2_copy(0, p).wait_send()
        for k in (2 * B - 2, 2 * B - 1):
            for kind in (0, 1, 3):
                piece(k, p, kind).wait_send()


EVENTS = {
    "norm": ((1, "e1", 0), (2, "e1", 1), (3, "e1", 2)),
    "attn": ((3, "e3", 1),),
    "wo": ((7, "e2", 0), (11, "e2", 1), (14, "e4", 0), (16, "e5", 0)),
    "qkv": ((6, "e3", 0),),
    "gu": ((0, "e1", 3), (1, "e2", 2), (2, "e4", 1), (11, "e2", 3), (12, "e3", 2), (13, "e1", 4), (16, "e4", 3), (21, "e5", 2), (26, "e1", 5), (27, "e4", 4), (34, "e2", 5), (37, "e5", 4), (39, "e1", 6), (40, "e5", 5), (45, "e2", 6), (49, "e3", 6)),
    "down": ((2, "e5", 1), (4, "ld", 1), (6, "e3", 3), (9, "e4", 2), (10, "e2", 4), (10, "ld", 2), (14, "e5", 3), (17, "e3", 4), (20, "e3", 5), (20, "ld", 3), (25, "e4", 5), (32, "e4", 6), (38, "e5", 6)),
    "m": ((0, "ld", 0),),
    "end": (("e1", 7), ("e2", 7), ("e3", 7), ("e4", 7), ("e5", 7)),
    "order": ("e5", "e4", "e3", "e2", "e1", "ld"),
}


def solution(mesh):
    def step(x, gain_a, wq, wk, wv, wo, gain_m, w_gate, w_up, w_down):
        half = HEAD // 2
        angle = jnp.arange(T, dtype=F32)[:, None] * THETA ** (-jnp.arange(half, dtype=F32) / half)
        cos, sin = jnp.cos(angle), jnp.sin(angle)
        anywhere, vmem = pl.BlockSpec(memory_space=pl.ANY), pl.BlockSpec(memory_space=pltpu.VMEM)
        dma = pltpu.SemaphoreType.DMA
        z = pl.pallas_call(
            functools.partial(_kernel, EVENTS),
            out_shape=jax.ShapeDtypeStruct((2 * B * T, D), BF),
            in_specs=[anywhere, vmem, anywhere, anywhere, anywhere, anywhere, vmem, anywhere, anywhere, anywhere, vmem, vmem],
            out_specs=pl.BlockSpec(memory_space=pltpu.HBM),
            scratch_shapes=[
                pltpu.VMEM((T, D), BF), pltpu.VMEM((T, FF), BF), pltpu.VMEM((HEAD, T), BF),
                pltpu.VMEM((2, D, 512), BF), pltpu.VMEM((NS, FF, 512), BF),
                pltpu.VMEM((256, D), F32), pltpu.VMEM((256, D), BF), pltpu.VMEM((2, 256, D), BF),
                pltpu.VMEM((2, 128, D), F32), pltpu.VMEM((128, D), BF), pltpu.VMEM((2, 128, D), BF),
                pltpu.VMEM((64, D), BF), pltpu.VMEM((2, 64, D), BF),
                pltpu.VMEM((2, 64, D), BF), pltpu.VMEM((B, 64, D), BF), pltpu.VMEM((2, 64, D), BF), pltpu.VMEM((4, 64, D), BF),
                dma((2, 2)), dma((NS, 2)), dma((DN,)), dma((2, DN)), dma((2,)), dma((2, 2)), dma((2,)), dma((2, 2)),
                dma((2 * B, 2, 7)), dma((2 * B, 2, 6)), dma((4,)), dma((2, 2)), dma(()),
            ],
            compiler_params=pltpu.CompilerParams(collective_id=0, has_side_effects=True, vmem_limit_bytes=VMEM),
            name="layer",
        )(x.reshape(B * T, D), gain_a.reshape(1, D), wq, wk, wv, wo, gain_m.reshape(1, D), w_gate, w_up, w_down,
          jnp.concatenate([cos, cos], -1), jnp.concatenate([-sin, sin], -1))
        return z[B * T :].reshape(x.shape)

    tokens, whole, columns, rows_of = P("dp", None, None), P(None), P(None, "tp"), P("tp", None)
    return jax.shard_map(
        step,
        mesh=mesh,
        in_specs=(tokens, whole, columns, columns, columns, rows_of, whole, columns, columns, rows_of),
        out_specs=tokens,
        check_vma=False,
    )
```
